128 devices in a mesh: pz: 4 (over z), py: 4 (over y), px: 8 (over x, core).
Axes of the slice: x: 4, y: 4, z: 4, core: 2. Of those that a mesh axis runs over, the one named last changes fastest.
Arguments:
- shift_diag: float32 [2, 384, 192, 384], P(None, 'px', 'py', 'pz')
- rhs_field: float32 [2, 384, 192, 384], P(None, 'px', 'py', 'pz')
- x_start: float32 [2, 384, 192, 384], P(None, 'px', 'py', 'pz')
- cond_x: float32 [2, 384, 192, 384], P(None, 'px', 'py', 'pz')
- cond_y: float32 [2, 384, 192, 384], P(None, 'px', 'py', 'pz')
- cond_z: float32 [2, 384, 192, 384], P(None, 'px', 'py', 'pz')
Outputs:
- output 1: float32 [2, 384, 192, 384], P(None, 'px', 'py', 'pz')
- output 2: float32 [2, 21], replicated
All inputs are finite; a program needn't handle non-finite values.
Results may differ from the reference program's by a relative error of at most 0.001.
Values sent between devices are 32-bit elements.
A program may use at most 1 GiB of HBM per device.

```python
import jax
import jax.numpy as jnp
from jax import lax

GRID_X = 384
GRID_Y = 192
GRID_Z = 384
ITERS = 20


def setup_inputs(seed: int = 0) -> dict:
    base_key = jax.random.key(seed)
    sub_keys = jax.random.split(base_key, 6)
    field_shape = (2, GRID_X, GRID_Y, GRID_Z)
    shift_diag = 0.05 + 0.3 * jax.random.uniform(sub_keys[0], field_shape, jnp.float32)
    rhs_field = jax.random.normal(sub_keys[1], field_shape, jnp.float32)
    x_start = 0.5 * jax.random.normal(sub_keys[2], field_shape, jnp.float32)
    cond_x = 0.1 + 1.8 * jax.random.uniform(sub_keys[3], field_shape, jnp.float32)
    cond_y = 0.1 + 1.8 * jax.random.uniform(sub_keys[4], field_shape, jnp.float32)
    cond_z = 0.1 + 1.8 * jax.random.uniform(sub_keys[5], field_shape, jnp.float32)
    return {'shift_diag': shift_diag, 'rhs_field': rhs_field, 'x_start': x_start, 'cond_x': cond_x, 'cond_y': cond_y, 'cond_z': cond_z}


def face_term(field, conduct, axis_dim):
    planes = field.shape[axis_dim]
    face_flux = lax.slice_in_dim(conduct, 0, planes - 1, axis=axis_dim) * (lax.slice_in_dim(field, 0, planes - 1, axis=axis_dim) - lax.slice_in_dim(field, 1, planes, axis=axis_dim))
    widths = [(1, 1) if pos_dim == axis_dim else (0, 0) for pos_dim in range(field.ndim)]
    padded = jnp.pad(face_flux, widths)
    return lax.slice_in_dim(padded, 1, planes + 1, axis=axis_dim) - lax.slice_in_dim(padded, 0, planes, axis=axis_dim)


def apply_operator(field, shift_diag, cond_x, cond_y, cond_z):
    return shift_diag * field + face_term(field, cond_x, 0) + face_term(field, cond_y, 1) + face_term(field, cond_z, 2)


def solve_one(fields):
    shift_diag, rhs_field, x_start, cond_x, cond_y, cond_z = fields
    cell_count = GRID_X * GRID_Y * GRID_Z
    residual = rhs_field - apply_operator(x_start, shift_diag, cond_x, cond_y, cond_z)
    rho_start = jnp.sum(residual * residual)

    def cg_step(loop_state, unused):
        x_cur, res_cur, direction, rho_old, beta_coef = loop_state
        direction = res_cur + beta_coef * direction
        q_vec = apply_operator(direction, shift_diag, cond_x, cond_y, cond_z)
        alpha_step = rho_old / jnp.sum(direction * q_vec)
        x_cur = x_cur + alpha_step * direction
        res_cur = res_cur - alpha_step * q_vec
        rho_new = jnp.sum(res_cur * res_cur)
        return (x_cur, res_cur, direction, rho_new, rho_new / rho_old), jnp.sqrt(rho_new / cell_count)

    init_state = (x_start, residual, jnp.zeros_like(residual), rho_start, jnp.zeros_like(rho_start))
    final_state, res_tail = lax.scan(cg_step, init_state, None, length=ITERS)
    res_hist = jnp.concatenate([jnp.sqrt(rho_start / cell_count)[None], res_tail])
    return final_state[0], res_hist


def reference(shift_diag, rhs_field, x_start, cond_x, cond_y, cond_z):
    x_final, res_hist = lax.map(solve_one, (shift_diag, rhs_field, x_start, cond_x, cond_y, cond_z))
    return x_final, res_hist
```

```python
import functools
import itertools

import jax
import jax.numpy as jnp
from jax import lax
from jax.experimental import pallas as pl
from jax.experimental.pallas import tpu as pltpu
from jax.sharding import PartitionSpec as P

ITERS = 20
SYS = 2
ROW0 = 8
LANES = 128
MESH = pl.DeviceIdType.MESH
PQ, RR, RR0 = 0, 1, 2


def far_first(nx, ny, nz):
    def route(offset):
        hops = sum(min(step, size - step) for step, size in zip(offset[1:], (nx // 2, ny, nz)))
        return (hops, offset[0])
    offsets = [offset for offset in itertools.product(range(2), range(nx // 2), range(ny), range(nz)) if any(offset)]
    return sorted(offsets, key=route, reverse=True)


def cg_kernel(axis_sizes, block, cell_count,
              s_ref, b_ref, x0_ref, kx_ref, ky_ref, kz_ref,
              x_ref, hist_out,
              r, p, q, kyd, kze, kx0,
              dot_send, dot_recv, rho_ref, beta_ref, hist_ref,
              y_send, y_recv, z_send, z_recv,
              yi_send, yi_recv, zi_send, zi_recv,
              dot_ssem, dot_rsem, halo_ssem, halo_rsem, init_ssem, init_rsem):
    nx, ny, nz = axis_sizes
    bx, by, bz = block
    n_dev = nx * ny * nz
    px, py, pz = lax.axis_index('px'), lax.axis_index('py'), lax.axis_index('pz')
    me = (pz * ny + py) * nx + px
    rows = pl.ds(ROW0, by)
    half = bx // 2
    lane_plane = lax.broadcasted_iota(jnp.int32, (by, LANES), 1)
    lane_row = lax.broadcasted_iota(jnp.int32, (1, LANES), 1)

    def device(x_pos, y_pos, z_pos):
        return {'px': x_pos, 'py': y_pos, 'pz': z_pos}

    x_up, x_dn = device(lax.rem(px + 1, nx), py, pz), device(lax.rem(px + nx - 1, nx), py, pz)
    y_up, y_dn = device(px, lax.rem(py + 1, ny), pz), device(px, lax.rem(py + ny - 1, ny), pz)
    z_up, z_dn = device(px, py, lax.rem(pz + 1, nz)), device(px, py, lax.rem(pz + nz - 1, nz))

    core, chip = lax.rem(px, 2), lax.div(px, 2)
    part_z = [lax.rem(pz + step, nz) for step in range(nz)]
    part_y = [lax.rem(py + step, ny) for step in range(ny)]
    part_x = [[lax.rem(chip + step, nx // 2) * 2 + lax.rem(core + flip, 2) for step in range(nx // 2)] for flip in range(2)]
    targets = far_first(nx, ny, nz)

    def remote(src, dst, send_sem, recv_sem, dev):
        return pltpu.make_async_remote_copy(src_ref=src, dst_ref=dst, send_sem=send_sem, recv_sem=recv_sem, device_id=dev, device_id_type=MESH)

    def dot_start(c, slot, acc):
        total = jnp.sum(jnp.sum(acc, axis=0, keepdims=True), axis=1, keepdims=True)
        row = jnp.broadcast_to(total, (1, LANES))
        dot_send[c, slot] = row
        dot_recv[c, slot, me] = row
        for flip, step_x, step_y, step_z in targets:
            dev = device(part_x[flip][step_x], part_y[step_y], part_z[step_z])
            remote(dot_send.at[c, slot], dot_recv.at[c, slot, me], dot_ssem.at[c, slot], dot_rsem.at[c, slot], dev).start()

    def dot_wait(c, slot):
        others = dot_recv.at[c, slot, pl.ds(0, n_dev - 1)]
        pltpu.make_async_copy(others, others, dot_rsem.at[c, slot]).wait()
        pltpu.make_async_copy(others, others, dot_ssem.at[c, slot]).wait()
        return jnp.sum(dot_recv[c, slot], axis=0)

    def z_shift(a):
        return a + 33 + jnp.where(a >= half, 64 - half, 0)

    def z_extract(load):
        def body(a, packed):
            shift = z_shift(a)
            moved = pltpu.roll(load(a), shift, 1)
            pick = jnp.logical_or(lane_plane == shift, lane_plane == shift - 33)
            return jnp.where(pick, moved, packed)
        return lax.fori_loop(0, bx, body, jnp.zeros((by, LANES), jnp.float32), unroll=4)

    def z_insert(own, from_dn, from_up, store):
        from_dn = jnp.where(pz == 0, pltpu.roll(own, LANES - 33, 1), from_dn)
        from_up = jnp.where(pz == nz - 1, pltpu.roll(own, 33, 1), from_up)
        low_lanes = jnp.logical_or(jnp.logical_and(lane_plane >= 33, lane_plane < 33 + half),
                                   jnp.logical_and(lane_plane >= 97, lane_plane < 97 + half))
        both = jnp.where(low_lanes, from_up, pltpu.roll(from_dn, 64, 1))

        def body(a, carry):
            moved = pltpu.roll(both, lax.rem(96 + LANES - z_shift(a), LANES), 1)
            store(a, moved[:, bz:])
            return carry
        lax.fori_loop(0, bx, body, 0, unroll=4)

    def halo_copies(c, field, ys, yr, zs, zr, ssem, rsem):
        return [
            remote(field.at[c, 1, rows], field.at[c, bx + 1, rows], ssem.at[c, 0], rsem.at[c, 0], x_dn),
            remote(field.at[c, bx, rows], field.at[c, 0, rows], ssem.at[c, 1], rsem.at[c, 1], x_up),
            remote(ys.at[c, 0], yr.at[c, 0], ssem.at[c, 2], rsem.at[c, 2], y_dn),
            remote(ys.at[c, 1], yr.at[c, 1], ssem.at[c, 3], rsem.at[c, 3], y_up),
            remote(zs.at[c], zr.at[c, 0], ssem.at[c, 4], rsem.at[c, 4], z_dn),
            remote(zs.at[c], zr.at[c, 1], ssem.at[c, 5], rsem.at[c, 5], z_up),
        ]

    def halo_start(c, field, ys, yr, zs, zr, ssem, rsem):
        copies = halo_copies(c, field, ys, yr, zs, zr, ssem, rsem)
        copies[0].start()
        copies[1].start()

        def pack(a, carry):
            ys[c, 0, a] = field[c, a + 1, ROW0:ROW0 + 1, :]
            ys[c, 1, a] = field[c, a + 1, ROW0 + by - 1:ROW0 + by, :]
            return carry
        lax.fori_loop(0, bx, pack, 0, unroll=8)
        copies[2].start()
        copies[3].start()
        zs[c] = z_extract(lambda a: field[c, a + 1, ROW0:ROW0 + by, :])
        copies[4].start()
        copies[5].start()

    def halo_finish(c, field, ys, yr, zs, zr, ssem, rsem):
        for copy in halo_copies(c, field, ys, yr, zs, zr, ssem, rsem):
            copy.wait()

        @pl.when(px == nx - 1)
        def _():
            field[c, bx + 1, ROW0:ROW0 + by, :] = field[c, bx, ROW0:ROW0 + by, :]

        @pl.when(px == 0)
        def _():
            field[c, 0, ROW0:ROW0 + by, :] = field[c, 1, ROW0:ROW0 + by, :]

        def unpack(a, carry):
            field[c, a + 1, ROW0 + by:ROW0 + by + 1, :] = jnp.where(py == ny - 1, ys[c, 1, a], yr[c, 0, a])
            field[c, a + 1, ROW0 - 1:ROW0, :] = jnp.where(py == 0, ys[c, 0, a], yr[c, 1, a])
            return carry
        lax.fori_loop(0, bx, unpack, 0, unroll=8)

        def store(a, lanes):
            field[c, a + 1, ROW0:ROW0 + by, bz:] = lanes
        z_insert(zs[c], zr[c, 1], zr[c, 0], store)

    r_halo = (r, y_send, y_recv, z_send, z_recv, halo_ssem, halo_rsem)
    x_halo = (p, yi_send.at[0], yi_recv.at[0], zi_send.at[0], zi_recv.at[0], init_ssem.at[0], init_rsem.at[0])

    def apply(c, beta, with_dot):
        def direction(j):
            if beta is None:
                return p[c, j, ROW0:ROW0 + by, :]
            new = r[c, j] + beta * p[c, j]
            p[c, j] = new
            return new[ROW0:ROW0 + by, :]

        def flux_x(conduct, low, high):
            return conduct * (low[:, :bz] - high[:, :bz])

        below, first = direction(0), direction(1)

        def body(a, carry):
            here, flux_low, acc = carry
            above = direction(a + 2)
            mid = here[:, :bz]
            flux_high = flux_x(kx_ref[c, a], here, above)
            flux_y = ky_ref[c, a] * (mid - p[c, a + 1, ROW0 + 1:ROW0 + by + 1, :bz])
            flux_yd = kyd[c, a] * (p[c, a + 1, ROW0 - 1:ROW0 + by - 1, :bz] - mid)
            flux_z = kze[c, a] * (here - pltpu.roll(here, LANES - 1, 1))
            part_z_ = (flux_z - pltpu.roll(flux_z, 1, 1))[:, :bz]
            out = s_ref[c, a] * mid + (flux_high - flux_low) + (flux_y - flux_yd) + part_z_
            q[c, a] = out
            if with_dot:
                acc = acc + mid * out
            return above, flux_high, acc

        start = (first, flux_x(kx0[c], below, first), jnp.zeros((by, bz), jnp.float32))
        return lax.fori_loop(0, bx, body, start)[2]

    def kx_copy(c):
        return remote(kx_ref.at[c, bx - 1], kx0.at[c], init_ssem.at[1, c, 0], init_rsem.at[1, c, 0], x_up)

    def ky_copy(c):
        return remote(yi_send.at[1, c, 0], yi_recv.at[1, c, 0], init_ssem.at[1, c, 1], init_rsem.at[1, c, 1], y_up)

    def kz_copy(c):
        return remote(zi_send.at[1, c], zi_recv.at[1, c, 0], init_ssem.at[1, c, 2], init_rsem.at[1, c, 2], z_up)

    for c in range(SYS):
        kx_copy(c).start()

        def fill(a, carry, c=c):
            value = x0_ref[c, a]
            x_ref[c, a] = value
            p[c, a + 1, ROW0:ROW0 + by, :bz] = value
            cond = ky_ref[c, a]
            kyd[c, a, 1:by, :] = cond[:by - 1, :]
            yi_send[1, c, 0, a, :, :bz] = cond[by - 1:by, :]
            kze[c, a, :, :bz] = kz_ref[c, a]
            return carry
        lax.fori_loop(0, bx, fill, 0)
        ky_copy(c).start()
        zi_send[1, c] = z_extract(lambda a, c=c: kze[c, a])
        kz_copy(c).start()
        halo_start(c, *x_halo)

    for c in range(SYS):
        rho_ref[c] = jnp.ones((1, LANES), jnp.float32)
        beta_ref[c] = jnp.zeros((1, LANES), jnp.float32)
        hist_ref[c] = jnp.zeros((1, LANES), jnp.float32)
        kx_copy(c).wait()
        ky_copy(c).wait()
        kz_copy(c).wait()

        def low_row(a, carry, c=c):
            kyd[c, a, 0:1, :] = yi_recv[1, c, 0, a, :, :bz]
            return carry
        lax.fori_loop(0, bx, low_row, 0, unroll=8)

        def store_low(a, lanes, c=c):
            kze[c, a, :, bz:] = lanes
        z_insert(zi_send[1, c], zi_recv[1, c, 0], zi_recv[1, c, 0], store_low)

    for c in range(SYS):
        halo_finish(c, *x_halo)
        apply(c, None, False)

        def first_residual(a, acc, c=c):
            res = b_ref[c, a] - q[c, a]
            r[c, a + 1, ROW0:ROW0 + by, :bz] = res
            return acc + res * res
        dot_start(c, RR0, lax.fori_loop(0, bx, first_residual, jnp.zeros((by, bz), jnp.float32)))
        halo_start(c, *r_halo)

    def record(c, k, rho):
        hist_ref[c] = jnp.where(lane_row == k, rho, hist_ref[c])

    def cg_step(k, carry):
        for c in range(SYS):
            halo_finish(c, *r_halo)

            @pl.when(k > 0)
            def _(c=c):
                rho = dot_wait(c, RR)
                beta_ref[c] = rho / rho_ref[c]
                rho_ref[c] = rho
                record(c, k, rho)
            dot_start(c, PQ, apply(c, beta_ref[c], True))

        alphas = []
        for c in range(SYS):
            @pl.when(k == 0)
            def _(c=c):
                rho = dot_wait(c, RR0)
                rho_ref[c] = rho
                record(c, 0, rho)
            alpha = rho_ref[c] / dot_wait(c, PQ)
            alphas.append(alpha)

            def residual(a, acc, c=c, alpha=alpha):
                res = r[c, a + 1, ROW0:ROW0 + by, :bz] - alpha[:, :bz] * q[c, a]
                r[c, a + 1, ROW0:ROW0 + by, :bz] = res
                return acc + res * res
            dot_start(c, RR, lax.fori_loop(0, bx, residual, jnp.zeros((by, bz), jnp.float32), unroll=2))
            halo_start(c, *r_halo)

        for c in range(SYS):
            def update(a, inner, c=c):
                x_ref[c, a] = x_ref[c, a] + alphas[c][:, :bz] * p[c, a + 1, ROW0:ROW0 + by, :bz]
                return inner
            lax.fori_loop(0, bx, update, 0, unroll=2)
        return carry

    lax.fori_loop(0, ITERS, cg_step, 0)

    for c in range(SYS):
        for copy in halo_copies(c, *r_halo):
            copy.wait()
        record(c, ITERS, dot_wait(c, RR))
        hist_out[c:c + 1, :] = jnp.sqrt(hist_ref[c] / cell_count)[:, :ITERS + 1]


def solution(mesh):
    axis_sizes = tuple(mesh.shape[axis_name] for axis_name in ('px', 'py', 'pz'))
    n_dev = axis_sizes[0] * axis_sizes[1] * axis_sizes[2]
    field_spec = P(None, 'px', 'py', 'pz')

    def local_solve(shift_diag, rhs_field, x_start, cond_x, cond_y, cond_z):
        block = x_start.shape[1:]
        bx, by, bz = block
        cell_count = bx * by * bz * n_dev
        f32 = jnp.float32
        vmem = pl.BlockSpec(memory_space=pltpu.VMEM)
        padded = (SYS, bx + 2, by + 2 * ROW0, LANES)
        scratch = [
            pltpu.VMEM(padded, f32), pltpu.VMEM(padded, f32),
            pltpu.VMEM((SYS,) + block, f32), pltpu.VMEM((SYS,) + block, f32),
            pltpu.VMEM((SYS, bx, by, LANES), f32), pltpu.VMEM((SYS, by, bz), f32),
            pltpu.VMEM((SYS, 3, 1, LANES), f32), pltpu.VMEM((SYS, 3, n_dev, 1, LANES), f32),
            pltpu.VMEM((SYS, 1, LANES), f32), pltpu.VMEM((SYS, 1, LANES), f32), pltpu.VMEM((SYS, 1, LANES), f32),
            pltpu.VMEM((SYS, 2, bx, 1, LANES), f32), pltpu.VMEM((SYS, 2, bx, 1, LANES), f32),
            pltpu.VMEM((SYS, by, LANES), f32), pltpu.VMEM((SYS, 2, by, LANES), f32),
            pltpu.VMEM((2, SYS, 2, bx, 1, LANES), f32), pltpu.VMEM((2, SYS, 2, bx, 1, LANES), f32),
            pltpu.VMEM((2, SYS, by, LANES), f32), pltpu.VMEM((2, SYS, 2, by, LANES), f32),
            pltpu.SemaphoreType.DMA((SYS, 3)), pltpu.SemaphoreType.DMA((SYS, 3)),
            pltpu.SemaphoreType.DMA((SYS, 6)), pltpu.SemaphoreType.DMA((SYS, 6)),
            pltpu.SemaphoreType.DMA((2, SYS, 6)), pltpu.SemaphoreType.DMA((2, SYS, 6)),
        ]
        return pl.pallas_call(
            functools.partial(cg_kernel, axis_sizes, block, float(cell_count)),
            out_shape=(jax.ShapeDtypeStruct(x_start.shape, f32), jax.ShapeDtypeStruct((SYS, ITERS + 1), f32)),
            in_specs=[vmem] * 6,
            out_specs=(vmem, vmem),
            scratch_shapes=scratch,
            compiler_params=pltpu.CompilerParams(has_side_effects=True, vmem_limit_bytes=62 * 1024 * 1024),
        )(shift_diag, rhs_field, x_start, cond_x, cond_y, cond_z)

    return jax.shard_map(local_solve, mesh=mesh, in_specs=(field_spec,) * 6, out_specs=(field_spec, P(None, None)), check_vma=False)
```

```python
import functools
import itertools

import jax
import jax.numpy as jnp
from jax import lax
from jax.experimental import pallas as pl
from jax.experimental.pallas import tpu as pltpu
from jax.sharding import PartitionSpec as P

ITERS = 20
SYS = 2
ROW0 = 8
LANES = 128
MESH = pl.DeviceIdType.MESH
AHEAD = 8
PQ, RR, RR0 = 0, 1, 2


def far_first(nx, ny, nz):
    def route(offset):
        hops = sum(min(step, size - step) for step, size in zip(offset[1:], (nx // 2, ny, nz)))
        return (hops, offset[0])
    offsets = [offset for offset in itertools.product(range(2), range(nx // 2), range(ny), range(nz)) if any(offset)]
    return sorted(offsets, key=route, reverse=True)


def cg_kernel(axis_sizes, block, cell_count,
              s_hbm, b_hbm, x0_hbm, kx_hbm, ky_hbm, kz_hbm,
              x_ref, hist_out,
              s_ref, b_ref, kx_ref, ky_ref, kz_ref,
              r, p, q, kyd, kze, kzd, kx0,
              dot_send, dot_recv, rho_ref, beta_ref, hist_ref,
              y_send, y_recv, z_send, z_recv,
              yi_send, yi_recv, zi_send, zi_recv,
              dot_ssem, dot_rsem, halo_ssem, halo_rsem, init_ssem, init_rsem, load_sem):
    nx, ny, nz = axis_sizes
    bx, by, bz = block
    n_dev = nx * ny * nz
    px, py, pz = lax.axis_index('px'), lax.axis_index('py'), lax.axis_index('pz')
    me = (pz * ny + py) * nx + px
    rows = pl.ds(ROW0, by)
    half = bx // 2
    lane_plane = lax.broadcasted_iota(jnp.int32, (by, LANES), 1)
    lane_row = lax.broadcasted_iota(jnp.int32, (1, LANES), 1)

    def device(x_pos, y_pos, z_pos):
        return {'px': x_pos, 'py': y_pos, 'pz': z_pos}

    x_up, x_dn = device(lax.rem(px + 1, nx), py, pz), device(lax.rem(px + nx - 1, nx), py, pz)
    y_up, y_dn = device(px, lax.rem(py + 1, ny), pz), device(px, lax.rem(py + ny - 1, ny), pz)
    z_up, z_dn = device(px, py, lax.rem(pz + 1, nz)), device(px, py, lax.rem(pz + nz - 1, nz))

    core, chip = lax.rem(px, 2), lax.div(px, 2)
    part_z = [lax.rem(pz + step, nz) for step in range(nz)]
    part_y = [lax.rem(py + step, ny) for step in range(ny)]
    part_x = [[lax.rem(chip + step, nx // 2) * 2 + lax.rem(core + flip, 2) for step in range(nx // 2)] for flip in range(2)]
    targets = far_first(nx, ny, nz)

    def remote(src, dst, send_sem, recv_sem, dev):
        return pltpu.make_async_remote_copy(src_ref=src, dst_ref=dst, send_sem=send_sem, recv_sem=recv_sem, device_id=dev, device_id_type=MESH)

    def dot_start(c, slot, acc):
        total = jnp.sum(jnp.sum(acc, axis=0, keepdims=True), axis=1, keepdims=True)
        row = jnp.broadcast_to(total, (1, LANES))
        dot_send[c, slot] = row
        dot_recv[c, slot, me] = row
        for flip, step_x, step_y, step_z in targets:
            dev = device(part_x[flip][step_x], part_y[step_y], part_z[step_z])
            remote(dot_send.at[c, slot], dot_recv.at[c, slot, me], dot_ssem.at[c, slot], dot_rsem.at[c, slot], dev).start()

    def dot_wait(c, slot):
        others = dot_recv.at[c, slot, pl.ds(0, n_dev - 1)]
        pltpu.make_async_copy(others, others, dot_rsem.at[c, slot]).wait()
        pltpu.make_async_copy(others, others, dot_ssem.at[c, slot]).wait()
        return jnp.sum(dot_recv[c, slot], axis=0)

    def z_shift(a):
        return a + 33 + jnp.where(a >= half, 64 - half, 0)

    def z_extract(load):
        def body(a, packed):
            shift = z_shift(a)
            moved = pltpu.roll(load(a), shift, 1)
            pick = jnp.logical_or(lane_plane == shift, lane_plane == shift - 33)
            return jnp.where(pick, moved, packed)
        return lax.fori_loop(0, bx, body, jnp.zeros((by, LANES), jnp.float32), unroll=4)

    def z_insert(own, from_dn, from_up, store):
        from_dn = jnp.where(pz == 0, pltpu.roll(own, LANES - 33, 1), from_dn)
        from_up = jnp.where(pz == nz - 1, pltpu.roll(own, 33, 1), from_up)
        low_lanes = jnp.logical_or(jnp.logical_and(lane_plane >= 33, lane_plane < 33 + half),
                                   jnp.logical_and(lane_plane >= 97, lane_plane < 97 + half))
        both = jnp.where(low_lanes, from_up, pltpu.roll(from_dn, 64, 1))

        def body(a, carry):
            moved = pltpu.roll(both, lax.rem(96 + LANES - z_shift(a), LANES), 1)
            store(a, moved[:, bz:])
            return carry
        lax.fori_loop(0, bx, body, 0, unroll=4)

    def halo_copies(c, field, ys, yr, zs, zr, ssem, rsem):
        return [
            remote(field.at[c, 1, rows], field.at[c, bx + 1, rows], ssem.at[c, 0], rsem.at[c, 0], x_dn),
            remote(field.at[c, bx, rows], field.at[c, 0, rows], ssem.at[c, 1], rsem.at[c, 1], x_up),
            remote(ys.at[c, 0], yr.at[c, 0], ssem.at[c, 2], rsem.at[c, 2], y_dn),
            remote(ys.at[c, 1], yr.at[c, 1], ssem.at[c, 3], rsem.at[c, 3], y_up),
            remote(zs.at[c], zr.at[c, 0], ssem.at[c, 4], rsem.at[c, 4], z_dn),
            remote(zs.at[c], zr.at[c, 1], ssem.at[c, 5], rsem.at[c, 5], z_up),
        ]

    def halo_start(c, field, ys, yr, zs, zr, ssem, rsem):
        copies = halo_copies(c, field, ys, yr, zs, zr, ssem, rsem)
        copies[0].start()
        copies[1].start()

        def pack(a, carry):
            ys[c, 0, a] = field[c, a + 1, ROW0:ROW0 + 1, :]
            ys[c, 1, a] = field[c, a + 1, ROW0 + by - 1:ROW0 + by, :]
            return carry
        lax.fori_loop(0, bx, pack, 0, unroll=8)
        copies[2].start()
        copies[3].start()
        zs[c] = z_extract(lambda a: field[c, a + 1, ROW0:ROW0 + by, :])
        copies[4].start()
        copies[5].start()

    def halo_finish(c, field, ys, yr, zs, zr, ssem, rsem):
        for copy in halo_copies(c, field, ys, yr, zs, zr, ssem, rsem):
            copy.wait()

        @pl.when(px == nx - 1)
        def _():
            field[c, bx + 1, ROW0:ROW0 + by, :] = field[c, bx, ROW0:ROW0 + by, :]

        @pl.when(px == 0)
        def _():
            field[c, 0, ROW0:ROW0 + by, :] = field[c, 1, ROW0:ROW0 + by, :]

        def unpack(a, carry):
            field[c, a + 1, ROW0 + by:ROW0 + by + 1, :] = jnp.where(py == ny - 1, ys[c, 1, a], yr[c, 0, a])
            field[c, a + 1, ROW0 - 1:ROW0, :] = jnp.where(py == 0, ys[c, 0, a], yr[c, 1, a])
            return carry
        lax.fori_loop(0, bx, unpack, 0, unroll=8)

        def store(a, lanes):
            field[c, a + 1, ROW0:ROW0 + by, bz:] = lanes
        z_insert(zs[c], zr[c, 1], zr[c, 0], store)

    r_halo = (r, y_send, y_recv, z_send, z_recv, halo_ssem, halo_rsem)
    x_halo = (p, yi_send.at[0], yi_recv.at[0], zi_send.at[0], zi_recv.at[0], init_ssem.at[0], init_rsem.at[0])

    def apply(c, beta, with_dot):
        def direction(j):
            if beta is None:
                return p[c, j, ROW0:ROW0 + by, :]
            new = r[c, j] + beta * p[c, j]
            p[c, j] = new
            return new[ROW0:ROW0 + by, :]

        def z_part(a):
            here = direction(a + 1)
            up = (here - pltpu.roll(here, LANES - 1, 1))[:, :bz]
            down = (pltpu.roll(here, 1, 1) - here)[:, :bz]
            q[c, a] = s_ref[c, a] * here[:, :bz] + (kz_ref[c, a] * up - kzd[c, a] * down)

        def xy_part(a, carry):
            mid, flux_low, acc = carry
            above = p[c, a + 2, ROW0:ROW0 + by, :bz]
            flux_high = kx_ref[c, a] * (mid - above)
            flux_y = ky_ref[c, a] * (mid - p[c, a + 1, ROW0 + 1:ROW0 + by + 1, :bz])
            flux_yd = kyd[c, a] * (p[c, a + 1, ROW0 - 1:ROW0 + by - 1, :bz] - mid)
            out = q[c, a] + (flux_high - flux_low) + (flux_y - flux_yd)
            q[c, a] = out
            if with_dot:
                acc = acc + mid * out
            return above, flux_high, acc

        def both(a, carry):
            z_part(a + AHEAD)
            return xy_part(a, carry)

        direction(0)
        direction(bx + 1)
        for a in range(AHEAD):
            z_part(a)
        first = p[c, 1, ROW0:ROW0 + by, :bz]
        carry = (first, kx0[c] * (p[c, 0, ROW0:ROW0 + by, :bz] - first), jnp.zeros((by, bz), jnp.float32))
        carry = lax.fori_loop(0, bx - AHEAD, both, carry, unroll=8)
        for a in range(bx - AHEAD, bx):
            carry = xy_part(a, carry)
        return carry[2]

    def load(c, i):
        pairs = ((x0_hbm, x_ref), (kx_hbm, kx_ref), (ky_hbm, ky_ref), (kz_hbm, kz_ref), (s_hbm, s_ref), (b_hbm, b_ref))
        src, dst = pairs[i]
        return pltpu.make_async_copy(src.at[c], dst.at[c], load_sem.at[c, i])

    for i in range(6):
        for c in range(SYS):
            load(c, i).start()

    barrier = pltpu.get_barrier_semaphore()
    for flip, step_x, step_y, step_z in targets:
        pl.semaphore_signal(barrier, inc=1, device_id=device(part_x[flip][step_x], part_y[step_y], part_z[step_z]), device_id_type=MESH)
    pl.semaphore_wait(barrier, n_dev - 1)

    def kx_copy(c):
        return remote(kx_ref.at[c, bx - 1], kx0.at[c], init_ssem.at[1, c, 0], init_rsem.at[1, c, 0], x_up)

    def ky_copy(c):
        return remote(yi_send.at[1, c, 0], yi_recv.at[1, c, 0], init_ssem.at[1, c, 1], init_rsem.at[1, c, 1], y_up)

    def kz_copy(c):
        return remote(zi_send.at[1, c], zi_recv.at[1, c, 0], init_ssem.at[1, c, 2], init_rsem.at[1, c, 2], z_up)

    for c in range(SYS):
        load(c, 0).wait()

        def fill_p(a, carry, c=c):
            p[c, a + 1, ROW0:ROW0 + by, :bz] = x_ref[c, a]
            return carry
        lax.fori_loop(0, bx, fill_p, 0, unroll=2)
        halo_start(c, *x_halo)

    for c in range(SYS):
        load(c, 1).wait()
        kx_copy(c).start()
        load(c, 2).wait()
        load(c, 3).wait()

        def fill(a, carry, c=c):
            cond = ky_ref[c, a]
            kyd[c, a, 1:by, :] = cond[:by - 1, :]
            yi_send[1, c, 0, a, :, :bz] = cond[by - 1:by, :]
            kze[c, a, :, :bz] = kz_ref[c, a]
            return carry
        lax.fori_loop(0, bx, fill, 0)
        ky_copy(c).start()
        zi_send[1, c] = z_extract(lambda a, c=c: kze[c, a])
        kz_copy(c).start()

    for c in range(SYS):
        rho_ref[c] = jnp.ones((1, LANES), jnp.float32)
        beta_ref[c] = jnp.zeros((1, LANES), jnp.float32)
        hist_ref[c] = jnp.zeros((1, LANES), jnp.float32)
        kx_copy(c).wait()
        ky_copy(c).wait()
        kz_copy(c).wait()

        def low_row(a, carry, c=c):
            kyd[c, a, 0:1, :] = yi_recv[1, c, 0, a, :, :bz]
            return carry
        lax.fori_loop(0, bx, low_row, 0, unroll=8)

        def store_low(a, lanes, c=c):
            kze[c, a, :, bz:] = lanes
        z_insert(zi_send[1, c], zi_recv[1, c, 0], zi_recv[1, c, 0], store_low)

        def shift_z(a, carry, c=c):
            kzd[c, a] = pltpu.roll(kze[c, a], 1, 1)[:, :bz]
            return carry
        lax.fori_loop(0, bx, shift_z, 0, unroll=8)

    for c in range(SYS):
        halo_finish(c, *x_halo)
        load(c, 4).wait()
        apply(c, None, False)
        load(c, 5).wait()

        def first_residual(a, acc, c=c):
            res = b_ref[c, a] - q[c, a]
            r[c, a + 1, ROW0:ROW0 + by, :bz] = res
            return acc + res * res
        dot_start(c, RR0, lax.fori_loop(0, bx, first_residual, jnp.zeros((by, bz), jnp.float32)))
        halo_start(c, *r_halo)

    def record(c, k, rho):
        hist_ref[c] = jnp.where(lane_row == k, rho, hist_ref[c])

    def cg_step(k, carry):
        for c in range(SYS):
            halo_finish(c, *r_halo)

            @pl.when(k > 0)
            def _(c=c):
                rho = dot_wait(c, RR)
                beta_ref[c] = rho / rho_ref[c]
                rho_ref[c] = rho
                record(c, k, rho)
            dot_start(c, PQ, apply(c, beta_ref[c], True))

        alphas = []
        for c in range(SYS):
            @pl.when(k == 0)
            def _(c=c):
                rho = dot_wait(c, RR0)
                rho_ref[c] = rho
                record(c, 0, rho)
            alpha = rho_ref[c] / dot_wait(c, PQ)
            alphas.append(alpha)

            def residual(a, acc, c=c, alpha=alpha):
                res = r[c, a + 1, ROW0:ROW0 + by, :bz] - alpha[:, :bz] * q[c, a]
                r[c, a + 1, ROW0:ROW0 + by, :bz] = res
                return acc + res * res
            dot_start(c, RR, lax.fori_loop(0, bx, residual, jnp.zeros((by, bz), jnp.float32), unroll=2))
            halo_start(c, *r_halo)

        for c in range(SYS):
            def update(a, inner, c=c):
                x_ref[c, a] = x_ref[c, a] + alphas[c][:, :bz] * p[c, a + 1, ROW0:ROW0 + by, :bz]
                return inner
            lax.fori_loop(0, bx, update, 0, unroll=2)
        return carry

    lax.fori_loop(0, ITERS, cg_step, 0)

    for c in range(SYS):
        for copy in halo_copies(c, *r_halo):
            copy.wait()
        record(c, ITERS, dot_wait(c, RR))
        hist_out[c:c + 1, :] = jnp.sqrt(hist_ref[c] / cell_count)[:, :ITERS + 1]


def solution(mesh):
    axis_sizes = tuple(mesh.shape[axis_name] for axis_name in ('px', 'py', 'pz'))
    n_dev = axis_sizes[0] * axis_sizes[1] * axis_sizes[2]
    field_spec = P(None, 'px', 'py', 'pz')

    def local_solve(shift_diag, rhs_field, x_start, cond_x, cond_y, cond_z):
        block = x_start.shape[1:]
        bx, by, bz = block
        cell_count = bx * by * bz * n_dev
        f32 = jnp.float32
        vmem = pl.BlockSpec(memory_space=pltpu.VMEM)
        padded = (SYS, bx + 2, by + 2 * ROW0, LANES)
        scratch = [
            *[pltpu.VMEM((SYS,) + block, f32)] * 5,
            pltpu.VMEM(padded, f32), pltpu.VMEM(padded, f32),
            pltpu.VMEM((SYS,) + block, f32), pltpu.VMEM((SYS,) + block, f32),
            pltpu.VMEM((SYS, bx, by, LANES), f32), pltpu.VMEM((SYS,) + block, f32),
            pltpu.VMEM((SYS, by, bz), f32),
            pltpu.VMEM((SYS, 3, 1, LANES), f32), pltpu.VMEM((SYS, 3, n_dev, 1, LANES), f32),
            pltpu.VMEM((SYS, 1, LANES), f32), pltpu.VMEM((SYS, 1, LANES), f32), pltpu.VMEM((SYS, 1, LANES), f32),
            pltpu.VMEM((SYS, 2, bx, 1, LANES), f32), pltpu.VMEM((SYS, 2, bx, 1, LANES), f32),
            pltpu.VMEM((SYS, by, LANES), f32), pltpu.VMEM((SYS, 2, by, LANES), f32),
            pltpu.VMEM((2, SYS, 2, bx, 1, LANES), f32), pltpu.VMEM((2, SYS, 2, bx, 1, LANES), f32),
            pltpu.VMEM((2, SYS, by, LANES), f32), pltpu.VMEM((2, SYS, 2, by, LANES), f32),
            pltpu.SemaphoreType.DMA((SYS, 3)), pltpu.SemaphoreType.DMA((SYS, 3)),
            pltpu.SemaphoreType.DMA((SYS, 6)), pltpu.SemaphoreType.DMA((SYS, 6)),
            pltpu.SemaphoreType.DMA((2, SYS, 6)), pltpu.SemaphoreType.DMA((2, SYS, 6)),
            pltpu.SemaphoreType.DMA((SYS, 6)),
        ]
        return pl.pallas_call(
            functools.partial(cg_kernel, axis_sizes, block, float(cell_count)),
            out_shape=(jax.ShapeDtypeStruct(x_start.shape, f32), jax.ShapeDtypeStruct((SYS, ITERS + 1), f32)),
            in_specs=[pl.BlockSpec(memory_space=pl.ANY)] * 6,
            out_specs=(vmem, vmem),
            scratch_shapes=scratch,
            compiler_params=pltpu.CompilerParams(has_side_effects=True, collective_id=0, vmem_limit_bytes=62 * 1024 * 1024),
        )(shift_diag, rhs_field, x_start, cond_x, cond_y, cond_z)

    return jax.shard_map(local_solve, mesh=mesh, in_specs=(field_spec,) * 6, out_specs=(field_spec, P(None, None)), check_vma=False)
```

```python
import functools
import itertools

import jax
import jax.numpy as jnp
from jax import lax
from jax.experimental import pallas as pl
from jax.experimental.pallas import tpu as pltpu
from jax.sharding import PartitionSpec as P

ITERS = 20
SYS = 2
ROW0 = 8
LANES = 128
MESH = pl.DeviceIdType.MESH
UNROLL = 12
PQ, RR, RR0 = 0, 1, 2


def far_first(nx, ny, nz):
    def route(offset):
        hops = sum(min(step, size - step) for step, size in zip(offset[1:], (nx // 2, ny, nz)))
        return (hops, offset[0])
    offsets = [offset for offset in itertools.product(range(2), range(nx // 2), range(ny), range(nz)) if any(offset)]
    return sorted(offsets, key=route, reverse=True)


def cg_kernel(axis_sizes, block, cell_count,
              s_hbm, b_hbm, x0_hbm, kx_hbm, ky_hbm, kz_hbm,
              x_ref, hist_out,
              s_ref, b_ref, kx_ref, ky_ref, kz_ref,
              r, p, q, kyd, kze, kzd, kx0,
              dot_send, dot_recv, rho_ref, beta_ref, hist_ref,
              y_send, y_recv, z_send, z_recv,
              yi_send, yi_recv, zi_send, zi_recv,
              dot_ssem, dot_rsem, halo_ssem, halo_rsem, init_ssem, init_rsem, load_sem):
    nx, ny, nz = axis_sizes
    bx, by, bz = block
    n_dev = nx * ny * nz
    px, py, pz = lax.axis_index('px'), lax.axis_index('py'), lax.axis_index('pz')
    me = (pz * ny + py) * nx + px
    rows = pl.ds(ROW0, by)
    half = bx // 2
    lane_plane = lax.broadcasted_iota(jnp.int32, (by, LANES), 1)
    lane_row = lax.broadcasted_iota(jnp.int32, (1, LANES), 1)

    def device(x_pos, y_pos, z_pos):
        return {'px': x_pos, 'py': y_pos, 'pz': z_pos}

    x_up, x_dn = device(lax.rem(px + 1, nx), py, pz), device(lax.rem(px + nx - 1, nx), py, pz)
    y_up, y_dn = device(px, lax.rem(py + 1, ny), pz), device(px, lax.rem(py + ny - 1, ny), pz)
    z_up, z_dn = device(px, py, lax.rem(pz + 1, nz)), device(px, py, lax.rem(pz + nz - 1, nz))

    core, chip = lax.rem(px, 2), lax.div(px, 2)
    part_z = [lax.rem(pz + step, nz) for step in range(nz)]
    part_y = [lax.rem(py + step, ny) for step in range(ny)]
    part_x = [[lax.rem(chip + step, nx // 2) * 2 + lax.rem(core + flip, 2) for step in range(nx // 2)] for flip in range(2)]
    targets = far_first(nx, ny, nz)

    def remote(src, dst, send_sem, recv_sem, dev):
        return pltpu.make_async_remote_copy(src_ref=src, dst_ref=dst, send_sem=send_sem, recv_sem=recv_sem, device_id=dev, device_id_type=MESH)

    def dot_start(c, slot, acc):
        total = jnp.sum(jnp.sum(acc, axis=0, keepdims=True), axis=1, keepdims=True)
        row = jnp.broadcast_to(total, (1, LANES))
        dot_send[c, slot] = row
        dot_recv[c, slot, me] = row
        for flip, step_x, step_y, step_z in targets:
            dev = device(part_x[flip][step_x], part_y[step_y], part_z[step_z])
            remote(dot_send.at[c, slot], dot_recv.at[c, slot, me], dot_ssem.at[c, slot], dot_rsem.at[c, slot], dev).start()

    def dot_wait(c, slot):
        others = dot_recv.at[c, slot, pl.ds(0, n_dev - 1)]
        pltpu.make_async_copy(others, others, dot_rsem.at[c, slot]).wait()
        pltpu.make_async_copy(others, others, dot_ssem.at[c, slot]).wait()
        terms = [dot_recv[c, slot, i] for i in range(n_dev)]
        while len(terms) > 1:
            terms = [low + high for low, high in zip(terms[0::2], terms[1::2])]
        return terms[0]

    def z_shift(a):
        return a + 33 + jnp.where(a >= half, 64 - half, 0)

    def z_extract(load):
        def body(a, packed):
            shift = z_shift(a)
            moved = pltpu.roll(load(a), shift, 1)
            pick = jnp.logical_or(lane_plane == shift, lane_plane == shift - 33)
            return jnp.where(pick, moved, packed)
        return lax.fori_loop(0, bx, body, jnp.zeros((by, LANES), jnp.float32), unroll=4)

    def z_insert(own, from_dn, from_up, store):
        from_dn = jnp.where(pz == 0, pltpu.roll(own, LANES - 33, 1), from_dn)
        from_up = jnp.where(pz == nz - 1, pltpu.roll(own, 33, 1), from_up)
        low_lanes = jnp.logical_or(jnp.logical_and(lane_plane >= 33, lane_plane < 33 + half),
                                   jnp.logical_and(lane_plane >= 97, lane_plane < 97 + half))
        both = jnp.where(low_lanes, from_up, pltpu.roll(from_dn, 64, 1))

        def body(a, carry):
            moved = pltpu.roll(both, lax.rem(96 + LANES - z_shift(a), LANES), 1)
            store(a, moved[:, bz:])
            return carry
        lax.fori_loop(0, bx, body, 0, unroll=4)

    def halo_copies(c, field, ys, yr, zs, zr, ssem, rsem):
        return [
            remote(field.at[c, 1, rows], field.at[c, bx + 1, rows], ssem.at[c, 0], rsem.at[c, 0], x_dn),
            remote(field.at[c, bx, rows], field.at[c, 0, rows], ssem.at[c, 1], rsem.at[c, 1], x_up),
            remote(ys.at[c, 0], yr.at[c, 0], ssem.at[c, 2], rsem.at[c, 2], y_dn),
            remote(ys.at[c, 1], yr.at[c, 1], ssem.at[c, 3], rsem.at[c, 3], y_up),
            remote(zs.at[c], zr.at[c, 0], ssem.at[c, 4], rsem.at[c, 4], z_dn),
            remote(zs.at[c], zr.at[c, 1], ssem.at[c, 5], rsem.at[c, 5], z_up),
        ]

    def halo_start(c, field, ys, yr, zs, zr, ssem, rsem, send=True):
        copies = halo_copies(c, field, ys, yr, zs, zr, ssem, rsem) if send else []

        def start(which):
            for copy in copies[which:which + 2]:
                copy.start()
        start(0)

        def pack(a, carry):
            ys[c, 0, a] = field[c, a + 1, ROW0:ROW0 + 1, :]
            ys[c, 1, a] = field[c, a + 1, ROW0 + by - 1:ROW0 + by, :]
            return carry
        lax.fori_loop(0, bx, pack, 0, unroll=8)
        start(2)
        zs[c] = z_extract(lambda a: field[c, a + 1, ROW0:ROW0 + by, :])
        start(4)

    def halo_finish(c, field, ys, yr, zs, zr, ssem, rsem):
        for copy in halo_copies(c, field, ys, yr, zs, zr, ssem, rsem):
            copy.wait()

        @pl.when(px == nx - 1)
        def _():
            field[c, bx + 1, ROW0:ROW0 + by, :] = field[c, bx, ROW0:ROW0 + by, :]

        @pl.when(px == 0)
        def _():
            field[c, 0, ROW0:ROW0 + by, :] = field[c, 1, ROW0:ROW0 + by, :]

        def unpack(a, carry):
            field[c, a + 1, ROW0 + by:ROW0 + by + 1, :] = jnp.where(py == ny - 1, ys[c, 1, a], yr[c, 0, a])
            field[c, a + 1, ROW0 - 1:ROW0, :] = jnp.where(py == 0, ys[c, 0, a], yr[c, 1, a])
            return carry
        lax.fori_loop(0, bx, unpack, 0, unroll=8)

        def store(a, lanes):
            field[c, a + 1, ROW0:ROW0 + by, bz:] = lanes
        z_insert(zs[c], zr[c, 1], zr[c, 0], store)

    r_halo = (r, y_send, y_recv, z_send, z_recv, halo_ssem, halo_rsem)
    x_halo = (p, yi_send.at[0], yi_recv.at[0], zi_send.at[0], zi_recv.at[0], init_ssem.at[0], init_rsem.at[0])

    def apply(c, beta, with_dot):
        def direction(j):
            if beta is None:
                return p[c, j, ROW0:ROW0 + by, :]
            new = r[c, j] + beta * p[c, j]
            p[c, j] = new
            return new[ROW0:ROW0 + by, :]

        def body(a, carry):
            here, flux_low, acc = carry
            above = direction(a + 2)
            mid = here[:, :bz]
            up = (here - pltpu.roll(here, LANES - 1, 1))[:, :bz]
            down = (pltpu.roll(here, 1, 1) - here)[:, :bz]
            flux_high = kx_ref[c, a] * (mid - above[:, :bz])
            flux_y = ky_ref[c, a] * (mid - p[c, a + 1, ROW0 + 1:ROW0 + by + 1, :bz])
            flux_yd = kyd[c, a] * (p[c, a + 1, ROW0 - 1:ROW0 + by - 1, :bz] - mid)
            out = s_ref[c, a] * mid + (flux_high - flux_low) + (flux_y - flux_yd) + (kz_ref[c, a] * up - kzd[c, a] * down)
            q[c, a] = out
            if with_dot:
                acc = acc + mid * out
            return above, flux_high, acc

        below, first = direction(0), direction(1)
        carry = (first, kx0[c] * (below[:, :bz] - first[:, :bz]), jnp.zeros((by, bz), jnp.float32))
        return lax.fori_loop(0, bx, body, carry, unroll=UNROLL)[2]

    def load(c, i):
        pairs = ((x0_hbm, x_ref), (kx_hbm, kx_ref), (ky_hbm, ky_ref), (kz_hbm, kz_ref), (s_hbm, s_ref), (b_hbm, b_ref))
        src, dst = pairs[i]
        return pltpu.make_async_copy(src.at[c], dst.at[c], load_sem.at[c, i])

    for i in range(6):
        for c in range(SYS):
            load(c, i).start()

    barrier = pltpu.get_barrier_semaphore()
    for flip, step_x, step_y, step_z in targets:
        pl.semaphore_signal(barrier, inc=1, device_id=device(part_x[flip][step_x], part_y[step_y], part_z[step_z]), device_id_type=MESH)
    def kx_copy(c):
        return remote(kx_ref.at[c, bx - 1], kx0.at[c], init_ssem.at[1, c, 0], init_rsem.at[1, c, 0], x_up)

    def ky_copy(c):
        return remote(yi_send.at[1, c, 0], yi_recv.at[1, c, 0], init_ssem.at[1, c, 1], init_rsem.at[1, c, 1], y_up)

    def kz_copy(c):
        return remote(zi_send.at[1, c], zi_recv.at[1, c, 0], init_ssem.at[1, c, 2], init_rsem.at[1, c, 2], z_up)

    for c in range(SYS):
        load(c, 0).wait()

        def fill_p(a, carry, c=c):
            p[c, a + 1, ROW0:ROW0 + by, :bz] = x_ref[c, a]
            return carry
        lax.fori_loop(0, bx, fill_p, 0, unroll=2)
        halo_start(c, *x_halo, send=False)

    for c in range(SYS):
        load(c, 1).wait()
        load(c, 2).wait()
        load(c, 3).wait()

        def fill(a, carry, c=c):
            cond = ky_ref[c, a]
            kyd[c, a, 1:by, :] = cond[:by - 1, :]
            yi_send[1, c, 0, a, :, :bz] = cond[by - 1:by, :]
            kze[c, a, :, :bz] = kz_ref[c, a]
            return carry
        lax.fori_loop(0, bx, fill, 0, unroll=4)
        zi_send[1, c] = z_extract(lambda a, c=c: kze[c, a])

    pl.semaphore_wait(barrier, n_dev - 1)
    for c in range(SYS):
        kx_copy(c).start()
        ky_copy(c).start()
        kz_copy(c).start()
        for copy in halo_copies(c, *x_halo):
            copy.start()

    for c in range(SYS):
        rho_ref[c] = jnp.ones((1, LANES), jnp.float32)
        beta_ref[c] = jnp.zeros((1, LANES), jnp.float32)
        hist_ref[c] = jnp.zeros((1, LANES), jnp.float32)
        kx_copy(c).wait()
        ky_copy(c).wait()
        kz_copy(c).wait()

        def low_row(a, carry, c=c):
            kyd[c, a, 0:1, :] = yi_recv[1, c, 0, a, :, :bz]
            return carry
        lax.fori_loop(0, bx, low_row, 0, unroll=8)

        def store_low(a, lanes, c=c):
            kze[c, a, :, bz:] = lanes
        z_insert(zi_send[1, c], zi_recv[1, c, 0], zi_recv[1, c, 0], store_low)

        def shift_z(a, carry, c=c):
            kzd[c, a] = pltpu.roll(kze[c, a], 1, 1)[:, :bz]
            return carry
        lax.fori_loop(0, bx, shift_z, 0, unroll=8)

    for c in range(SYS):
        halo_finish(c, *x_halo)
        load(c, 4).wait()
        apply(c, None, False)
        load(c, 5).wait()

        def first_residual(a, acc, c=c):
            res = b_ref[c, a] - q[c, a]
            r[c, a + 1, ROW0:ROW0 + by, :bz] = res
            return acc + res * res
        dot_start(c, RR0, lax.fori_loop(0, bx, first_residual, jnp.zeros((by, bz), jnp.float32), unroll=6))
        halo_start(c, *r_halo)

    def record(c, k, rho):
        hist_ref[c] = jnp.where(lane_row == k, rho, hist_ref[c])

    def cg_step(k, carry):
        for c in range(SYS):
            halo_finish(c, *r_halo)

            @pl.when(k > 0)
            def _(c=c):
                rho = dot_wait(c, RR)
                beta_ref[c] = rho / rho_ref[c]
                rho_ref[c] = rho
                record(c, k, rho)
            dot_start(c, PQ, apply(c, beta_ref[c], True))

        alphas = []
        for c in range(SYS):
            @pl.when(k == 0)
            def _(c=c):
                rho = dot_wait(c, RR0)
                rho_ref[c] = rho
                record(c, 0, rho)
            alpha = rho_ref[c] / dot_wait(c, PQ)
            alphas.append(alpha)

            def residual(a, acc, c=c, alpha=alpha):
                res = r[c, a + 1, ROW0:ROW0 + by, :bz] - alpha[:, :bz] * q[c, a]
                r[c, a + 1, ROW0:ROW0 + by, :bz] = res
                return acc + res * res
            dot_start(c, RR, lax.fori_loop(0, bx, residual, jnp.zeros((by, bz), jnp.float32), unroll=6))
            halo_start(c, *r_halo)

        for c in range(SYS):
            def update(a, inner, c=c):
                x_ref[c, a] = x_ref[c, a] + alphas[c][:, :bz] * p[c, a + 1, ROW0:ROW0 + by, :bz]
                return inner
            lax.fori_loop(0, bx, update, 0, unroll=2)
        return carry

    lax.fori_loop(0, ITERS, cg_step, 0)

    for c in range(SYS):
        for copy in halo_copies(c, *r_halo):
            copy.wait()
        record(c, ITERS, dot_wait(c, RR))
        hist_out[c:c + 1, :] = jnp.sqrt(hist_ref[c] / cell_count)[:, :ITERS + 1]


def solution(mesh):
    axis_sizes = tuple(mesh.shape[axis_name] for axis_name in ('px', 'py', 'pz'))
    n_dev = axis_sizes[0] * axis_sizes[1] * axis_sizes[2]
    field_spec = P(None, 'px', 'py', 'pz')

    def local_solve(shift_diag, rhs_field, x_start, cond_x, cond_y, cond_z):
        block = x_start.shape[1:]
        bx, by, bz = block
        cell_count = bx * by * bz * n_dev
        f32 = jnp.float32
        vmem = pl.BlockSpec(memory_space=pltpu.VMEM)
        padded = (SYS, bx + 2, by + 2 * ROW0, LANES)
        scratch = [
            *[pltpu.VMEM((SYS,) + block, f32)] * 5,
            pltpu.VMEM(padded, f32), pltpu.VMEM(padded, f32),
            pltpu.VMEM((SYS,) + block, f32), pltpu.VMEM((SYS,) + block, f32),
            pltpu.VMEM((SYS, bx, by, LANES), f32), pltpu.VMEM((SYS,) + block, f32),
            pltpu.VMEM((SYS, by, bz), f32),
            pltpu.VMEM((SYS, 3, 1, LANES), f32), pltpu.VMEM((SYS, 3, n_dev, 1, LANES), f32),
            pltpu.VMEM((SYS, 1, LANES), f32), pltpu.VMEM((SYS, 1, LANES), f32), pltpu.VMEM((SYS, 1, LANES), f32),
            pltpu.VMEM((SYS, 2, bx, 1, LANES), f32), pltpu.VMEM((SYS, 2, bx, 1, LANES), f32),
            pltpu.VMEM((SYS, by, LANES), f32), pltpu.VMEM((SYS, 2, by, LANES), f32),
            pltpu.VMEM((2, SYS, 2, bx, 1, LANES), f32), pltpu.VMEM((2, SYS, 2, bx, 1, LANES), f32),
            pltpu.VMEM((2, SYS, by, LANES), f32), pltpu.VMEM((2, SYS, 2, by, LANES), f32),
            pltpu.SemaphoreType.DMA((SYS, 3)), pltpu.SemaphoreType.DMA((SYS, 3)),
            pltpu.SemaphoreType.DMA((SYS, 6)), pltpu.SemaphoreType.DMA((SYS, 6)),
            pltpu.SemaphoreType.DMA((2, SYS, 6)), pltpu.SemaphoreType.DMA((2, SYS, 6)),
            pltpu.SemaphoreType.DMA((SYS, 6)),
        ]
        return pl.pallas_call(
            functools.partial(cg_kernel, axis_sizes, block, float(cell_count)),
            out_shape=(jax.ShapeDtypeStruct(x_start.shape, f32), jax.ShapeDtypeStruct((SYS, ITERS + 1), f32)),
            in_specs=[pl.BlockSpec(memory_space=pl.ANY)] * 6,
            out_specs=(vmem, vmem),
            scratch_shapes=scratch,
            compiler_params=pltpu.CompilerParams(has_side_effects=True, collective_id=0, vmem_limit_bytes=62 * 1024 * 1024),
        )(shift_diag, rhs_field, x_start, cond_x, cond_y, cond_z)

    return jax.shard_map(local_solve, mesh=mesh, in_specs=(field_spec,) * 6, out_specs=(field_spec, P(None, None)), check_vma=False)
```
